32 devices in a mesh: attn: 4 (over y, x), expert: 4 (over z), hid: 2 (over core).
Axes of the slice: x: 2, y: 2, z: 4, core: 2. Of those that a mesh axis runs over, the one named last changes fastest.
Arguments:
- residual: bfloat16 [8, 128, 2880], P(('attn', 'hid'), 'expert'), may hold values from -3 to 3
- queries: bfloat16 [1024, 4096], P(('attn', 'hid'), 'expert'), may hold values from -6 to 6
- cache_pairs: bfloat16 [1024, 8, 128, 128], P(('attn', 'hid'), 'expert'), may hold values from -6 to 6
- fresh_pairs: bfloat16 [1024, 8, 128], P(('attn', 'hid'), 'expert'), may hold values from -6 to 6
- cache_lengths: int32 [1024], P(('attn', 'hid')), may hold values from 1 to 1024, as said below
- sink_logits: float32 [64], P('expert'), may hold values from 1 to 6
- out_weight: bfloat16 [4096, 2880], P('expert'), may hold values from -0.375 to 0.375
- norm_gain: float32 [2880], replicated, may hold values from 0.1 to 1.9
- expert_index: int32 [8, 128, 4], P(('attn', 'hid'), 'expert'), may hold values from 0 to 31, all different within a row; in each aligned block of 32 rows (0 to 31, 32 to 63, ..., all dimensions but the last counted through in order) at most 8 rows name the same one
- route_weights: float32 [8, 128, 4], P(('attn', 'hid'), 'expert'), may hold values from 0.05 to 0.5
- gate_up_weight: bfloat16 [32, 2880, 2, 2880], P(('attn', 'hid'), None, None, 'expert'), may hold values from -0.109375 to 0.109375
- down_weight: bfloat16 [32, 2880, 2880], P(('attn', 'hid'), 'expert'), may hold values from -0.109375 to 0.109375
Outputs:
- layer_output: bfloat16 [8, 128, 2880], P(('attn', 'hid'), 'expert')
The draws below stay inside these ranges and needn't reach their ends.
Inputs may be any that keep to these rules, and one draw needn't show every extreme that they name: `expert_index`: each row names 4 different experts; in each aligned block of 32 rows (the tokens of one device) no expert is named more than 8 times, a bound that some block reaches. `cache_lengths`: both ends are reached in every draw.
All inputs are finite; a program needn't handle non-finite values.
Results may differ from the reference program's by a relative error of at most 0.013.
Values may be sent and summed in bfloat16 or wider, within the bound.
No kernel may reach another device: no remote copies, remote signals or barrier semaphores. Data moves between devices by JAX's collectives and lax.ppermute only.
A program may use at most 128 MiB of HBM per device.

```python
import math
import jax
import jax.numpy as jnp
import numpy as np
from jax import lax

D = 2880
HEADS = 64
KVH = 8
HD = 64
EXPERTS = 32
FF = 2880
TOP = 4
WINDOW = 128
CTX = 1024
SEQ_DEV = 128
GROUPS = 8
SEQS = 1024
ROWS = 32
MOST = 8
N_EXPERT = 4


def draw_queries(key, part):
    drawn = jnp.clip(jax.random.normal(jax.random.fold_in(key, 1), (SEQS, HEADS, HD), jnp.float32), -6.0, 6.0)
    return drawn.reshape(SEQS, HEADS * HD).astype(jnp.bfloat16)


def draw_cache_pairs(key, part):
    drawn = jnp.clip(jax.random.normal(jax.random.fold_in(key, 2), (SEQS, KVH, WINDOW, 2 * HD), jnp.float32), -6.0, 6.0)
    return drawn.astype(jnp.bfloat16)


def draw_fresh_pairs(key, part):
    drawn = jnp.clip(jax.random.normal(jax.random.fold_in(key, 3), (SEQS, KVH, 2 * HD), jnp.float32), -6.0, 6.0)
    return drawn.astype(jnp.bfloat16)


def draw_cache_lengths(key, part):
    key_a, key_b, key_c = jax.random.split(jax.random.fold_in(key, 4), 3)
    exponent = jax.random.randint(key_a, (SEQS,), 1, 11)
    ceiling = jnp.minimum(jnp.left_shift(jnp.ones_like(exponent), exponent), CTX)
    lengths = 1 + jax.random.randint(key_b, (SEQS,), 0, CTX) % ceiling
    picked = jax.random.randint(key_c, (), 0, SEQS)
    lengths = lengths.at[picked].set(CTX).at[(picked + 1) % SEQS].set(1)
    return lengths.astype(jnp.int32)


def block_levels(rng, extent, cuts, low, high):
    def one(axis_at, blocks):
        steps = jax.random.uniform(jax.random.fold_in(jax.random.fold_in(rng, 6), axis_at), (blocks,), jnp.float32, low / len(cuts), high / len(cuts))
        return jnp.repeat(jnp.exp(steps), extent[axis_at] // blocks).reshape((-1,) + (1,) * (len(extent) - axis_at - 1))

    loudness = one(*cuts[0])
    for cut in cuts[1:]:
        loudness = loudness * one(*cut)
    return loudness


def assign_block(own_key, own, number, rows, number_of, top, bound, lean):
    sequence = jax.random.permutation(own_key, number_of)
    crowded, common = load_shares(number_of, rows * top, bound, lean, True), load_shares(number_of, rows * top, bound, lean, False)
    places = jnp.arange(number_of)

    def named(sizes, rotation):
        used = int((sizes > 0).sum())
        fixed = max(1, used // 4)
        passed = fixed + (places - fixed + rotation * (used - fixed)) % max(1, number_of - fixed)
        return jnp.zeros((number_of,), jnp.int32).at[sequence[jnp.where(places < fixed, places, passed)]].set(jnp.asarray(sizes, jnp.int32))

    sizes = jnp.where(number % 4 == 0, named(crowded, number // 4), named(common, number - number // 4 - 1))
    mixed = jax.random.permutation(jax.random.fold_in(own, 3), number_of)
    donor, receiver = mixed[0:number_of // 2 * 2:2], mixed[1:number_of // 2 * 2:2]
    slack = jnp.minimum(sizes[donor] - 1, bound - sizes[receiver]) // 2
    slack = jnp.where((donor == sequence[0]) | (receiver == sequence[0]) | (sizes[receiver] == 0), 0, jnp.maximum(slack, 0))
    passed = jax.random.randint(jax.random.fold_in(own, 4), (number_of // 2,), 0, 1 << 20) % (slack + 1)
    sizes = sizes.at[donor].add(-passed).at[receiver].add(passed)
    labels = jnp.searchsorted(jnp.cumsum(sizes), jnp.arange(rows * top), side="right").astype(jnp.int32)
    grid = labels.reshape(top, rows).T
    grid = grid[jax.random.permutation(jax.random.fold_in(own, 1), rows)]
    rotation = jax.random.randint(jax.random.fold_in(own, 2), (rows, 1), 0, top)
    return jnp.take_along_axis(grid, (jnp.arange(top)[None, :] + rotation) % top, axis=1)


def load_shares(amount, total, limit, slope, full):
    loads = [(1 << 20) // math.isqrt(standing ** slope) + 1 for standing in range(1, amount + 1)]
    largest = limit if full else min(limit, max(-(-total // amount), total * loads[0] // sum(loads)))
    least = 1 if total - largest >= amount - 1 else 0
    given, surplus = [largest] + [least] * (amount - 1), total - largest - least * (amount - 1)
    while surplus > 0:
        candidates = [i for i in range(1, amount) if given[i] < largest] or [i for i in range(1, amount) if given[i] < limit]
        pool, remaining = sum([loads[i] for i in candidates]), surplus
        for i in candidates:
            more = min(limit - given[i], max(1, remaining * loads[i] // pool), surplus)
            given[i] = given[i] + more
            surplus = surplus - more
    return np.array(given)


def gaussian(stream_key, dims, spread, limit, shards=(), kind=jnp.bfloat16):
    loudness = block_levels(stream_key, dims, shards, -0.22, 0.18) if shards else 1.0
    result = jax.random.normal(stream_key, dims, jnp.float32) * spread * loudness
    return jnp.minimum(jnp.maximum(result, -limit), limit).astype(kind)


def setup_inputs(seed: int = 0) -> dict:
    seeds = jax.random.split(jax.random.key(seed), 13)
    residual = gaussian(seeds[0], (GROUPS, SEQ_DEV, D), 0.5, 3.0, ((0, 8), (1, 4)))
    queries = draw_queries(jax.random.fold_in(seeds[12], 71), 0)
    cache_pairs = draw_cache_pairs(jax.random.fold_in(seeds[12], 71), 0)
    fresh_pairs = draw_fresh_pairs(jax.random.fold_in(seeds[12], 71), 0)
    cache_lengths = draw_cache_lengths(jax.random.fold_in(seeds[12], 71), 0)
    sink_logits = jnp.clip(1.0 + 5.0 * jax.random.uniform(seeds[5], (HEADS,), jnp.float32) ** block_levels(seeds[5], (HEADS,), ((0, 4),), -0.2, 0.2), 1.0, 6.0)
    out_weight = gaussian(seeds[6], (HEADS * HD, D), (HEADS * HD // 16) ** -0.5, 0.375, ((0, 4),))
    norm_gain = jnp.clip(1.0 + 0.18 * jax.random.normal(seeds[7], (D,), jnp.float32), 0.1, 1.9)
    expert_index_keys = jax.random.split(jax.random.fold_in(seeds[8], 1), GROUPS * SEQ_DEV // ROWS)
    expert_index_turns = jax.random.permutation(jax.random.fold_in(seeds[8], 3), GROUPS * SEQ_DEV // ROWS)
    expert_index = jax.vmap(lambda own, number: assign_block(jax.random.fold_in(seeds[8], 2), own, number, ROWS, EXPERTS, TOP, MOST, 2))(expert_index_keys, expert_index_turns).reshape((GROUPS, SEQ_DEV, TOP))
    route_weights = jnp.clip(0.05 + 0.45 * jax.random.uniform(seeds[9], (GROUPS, SEQ_DEV, TOP), jnp.float32) ** block_levels(seeds[9], (GROUPS, SEQ_DEV, TOP), ((0, 8), (1, 4)), -0.2, 0.2), 0.05, 0.5)
    gate_up_weight = gaussian(seeds[10], (EXPERTS, D, 2, FF), D ** -0.5, 0.109375, ((0, 8), (3, 4)))
    down_weight = gaussian(seeds[11], (EXPERTS, FF, D), FF ** -0.5, 0.109375, ((0, 8), (1, 4)))
    return dict(residual=residual, queries=queries, cache_pairs=cache_pairs, fresh_pairs=fresh_pairs, cache_lengths=cache_lengths, sink_logits=sink_logits, out_weight=out_weight, norm_gain=norm_gain, expert_index=expert_index, route_weights=route_weights, gate_up_weight=gate_up_weight, down_weight=down_weight)


def attend(queries, cache_pairs, fresh_pairs, cache_lengths, sink_logits):
    group_size = HEADS // KVH
    grouped = queries.reshape(SEQS, KVH, group_size, HD).astype(jnp.float32)
    key_part = cache_pairs[..., :HD].astype(jnp.float32)
    value_part = cache_pairs[..., HD:].astype(jnp.float32)
    new_key = fresh_pairs[..., :HD].astype(jnp.float32)
    new_value = fresh_pairs[..., HD:].astype(jnp.float32)
    inv_root = 1.0 / math.sqrt(HD)
    scores = jnp.einsum('sjgd,sjtd->sjgt', grouped, key_part) * inv_root
    own_score = jnp.einsum('sjgd,sjd->sjg', grouped, new_key) * inv_root
    filled = jnp.minimum(cache_lengths, WINDOW).astype(jnp.int32)
    usable = (jnp.arange(WINDOW, dtype=jnp.int32)[None, :] < filled[:, None])[:, None, None, :]
    sink_bias = sink_logits.reshape(KVH, group_size)[None]
    largest = jnp.maximum(jnp.maximum(lax.optimization_barrier(jnp.max(jnp.where(usable, scores, -jnp.inf), axis=-1)), own_score), sink_bias)
    cache_exp = jnp.where(usable, jnp.exp(scores - largest[..., None]), 0.0)
    own_exp = jnp.exp(own_score - largest)
    denominator = lax.optimization_barrier(jnp.sum(cache_exp, axis=-1)) + own_exp + jnp.exp(sink_bias - largest)
    probabilities = (cache_exp / denominator[..., None]).astype(jnp.bfloat16)
    own_weight = (own_exp / denominator).astype(jnp.bfloat16)
    context = jnp.einsum('sjgt,sjtd->sjgd', probabilities.astype(jnp.float32), value_part)
    context = context + own_weight.astype(jnp.float32)[..., None] * new_value[:, :, None, :]
    return context.astype(jnp.bfloat16).reshape(SEQS, HEADS * HD)

def reference(residual, queries, cache_pairs, fresh_pairs, cache_lengths, sink_logits, out_weight, norm_gain, expert_index, route_weights, gate_up_weight, down_weight):
    context = attend(queries, cache_pairs, fresh_pairs, cache_lengths, sink_logits)
    attention = jnp.dot(context, out_weight, preferred_element_type=jnp.float32)
    middle = residual.astype(jnp.float32).reshape(SEQS, D) + attention
    normed = (middle * lax.rsqrt(lax.optimization_barrier(jnp.mean(middle * middle, axis=1, keepdims=True)) + 1e-05) * norm_gain).astype(jnp.bfloat16)
    chosen = expert_index.reshape(SEQS * TOP).astype(jnp.int32)
    capacity = GROUPS * N_EXPERT * MOST

    def one_expert(expert):
        routed = chosen == expert
        indices = jnp.nonzero(routed, size=capacity, fill_value=0)[0].astype(jnp.int32)
        present = jnp.arange(capacity, dtype=jnp.int32) < jnp.sum(routed.astype(jnp.int32))
        token_rows = normed[indices // TOP]
        merged = gate_up_weight[expert].reshape(D, 2 * FF)
        projected = jnp.dot(token_rows, merged, preferred_element_type=jnp.float32)
        gate_half = projected[:, :FF]
        up_half = projected[:, FF:]
        activation = ((up_half + 1.0) * gate_half * jax.nn.sigmoid(1.702 * gate_half)).astype(jnp.bfloat16)
        expert_out = jnp.dot(activation, down_weight[expert], preferred_element_type=jnp.float32).astype(jnp.bfloat16)
        return (indices, present, expert_out)
    indices, present, outputs = lax.map(one_expert, jnp.arange(EXPERTS, dtype=jnp.int32))
    kept = jnp.where(present.reshape(-1)[:, None], outputs.reshape(-1, D).astype(jnp.float32), 0.0)
    pair_out = jnp.zeros((SEQS * TOP, D), jnp.float32).at[indices.reshape(-1)].add(kept)
    weighted = pair_out.reshape(SEQS, TOP, D) * route_weights.reshape(SEQS, TOP)[:, :, None]
    layer_output = (middle + lax.optimization_barrier(jnp.sum(weighted, axis=1))).astype(jnp.bfloat16)
    return layer_output.reshape(GROUPS, SEQ_DEV, D)
```

```python
import math

import jax
import jax.numpy as jnp
from jax import lax
from jax.sharding import PartitionSpec as P

EXPERTS = 32
TOP = 4
EXTRA = 64


def attend(queries, cache_pairs, fresh_pairs, cache_lengths, sink_logits):
    seq_count, kv_heads, window_slots, doubled = cache_pairs.shape
    head_dim = doubled // 2
    group_size = queries.shape[1] // (kv_heads * head_dim)
    grouped = queries.reshape(seq_count, kv_heads, group_size, head_dim)
    inv_root = 1.0 / math.sqrt(head_dim)
    scores = (
        jnp.einsum(
            "sjgd,sjtd->sjgt",
            grouped,
            cache_pairs[..., :head_dim],
            preferred_element_type=jnp.float32,
        )
        * inv_root
    )
    own_score = (
        jnp.einsum(
            "sjgd,sjd->sjg",
            grouped,
            fresh_pairs[..., :head_dim],
            preferred_element_type=jnp.float32,
        )
        * inv_root
    )
    filled = jnp.minimum(cache_lengths, window_slots)
    usable = (jnp.arange(window_slots, dtype=jnp.int32)[None, :] < filled[:, None])[
        :, None, None, :
    ]
    sink_bias = sink_logits.reshape(kv_heads, group_size)[None]
    largest = jnp.maximum(
        jnp.maximum(jnp.max(jnp.where(usable, scores, -jnp.inf), axis=-1), own_score), sink_bias
    )
    cache_exp = jnp.where(usable, jnp.exp(scores - largest[..., None]), 0.0)
    own_exp = jnp.exp(own_score - largest)
    denominator = jnp.sum(cache_exp, axis=-1) + own_exp + jnp.exp(sink_bias - largest)
    probabilities = (cache_exp / denominator[..., None]).astype(jnp.bfloat16)
    own_weight = (own_exp / denominator).astype(jnp.bfloat16)
    context = jnp.einsum(
        "sjgt,sjtd->sjgd",
        probabilities,
        cache_pairs[..., head_dim:],
        preferred_element_type=jnp.float32,
    )
    context = context + own_weight.astype(jnp.float32)[..., None] * fresh_pairs[
        :, :, None, head_dim:
    ].astype(jnp.float32)
    return context.astype(jnp.bfloat16).reshape(seq_count, -1)


def swap(value, axis, bits):
    size = lax.axis_size(axis)
    return lax.ppermute(value, axis, [(i, i ^ bits) for i in range(size)])


def axis_bits(axis):
    size = lax.axis_size(axis)
    return [1 << b for b in range(size.bit_length() - 1)]


def gather_attn(block):
    half = block.shape[0] // 2
    bits = axis_bits("attn")
    parts = []
    for piece, order in ((block[:half], bits), (block[half:], bits[::-1])):
        held = {0: piece}
        for bit in order:
            offsets = sorted(held)
            sent = held[0][None] if len(offsets) == 1 else jnp.stack([held[o] for o in offsets])
            got = swap(sent, "attn", bit)
            for place, o in enumerate(offsets):
                held[o ^ bit] = got[place]
        parts.append([held[o] for o in range(1 << len(bits))])
    return jnp.stack([jnp.concatenate(pair) for pair in zip(*parts)])


def scatter_attn(block):
    half = block.shape[1] // 2
    bits = axis_bits("attn")
    parts = []
    for piece, order in ((block[:, :half], bits), (block[:, half:], bits[::-1])):
        held = {o: piece[o] for o in range(piece.shape[0])}
        for bit in order:
            kept = [o for o in sorted(held) if not o & bit]
            sent = jnp.stack([held[o ^ bit].astype(jnp.bfloat16) for o in kept])
            got = swap(sent, "attn", bit)
            held = {o: held[o] + got[place].astype(jnp.float32) for place, o in enumerate(kept)}
        parts.append(held[0])
    return jnp.concatenate(parts)


def on_device(
    residual,
    queries,
    cache_pairs,
    fresh_pairs,
    cache_lengths,
    sink_logits,
    out_weight,
    norm_gain,
    expert_index,
    route_weights,
    gate_up_weight,
    down_weight,
):
    deep = lax.axis_size("expert")
    wide = lax.axis_size("attn")
    cores = lax.axis_size("hid")
    place = lax.axis_index("expert")
    rows = residual.shape[1]
    width = residual.shape[2]

    context = attend(queries, cache_pairs, fresh_pairs, cache_lengths, sink_logits)
    by_place = context.reshape(deep, rows, -1)
    ordered = jnp.concatenate(
        [lax.dynamic_slice_in_dim(by_place, place ^ k, 1, 0) for k in range(deep)]
    ).reshape(deep * rows, -1)
    projected = jnp.dot(ordered, out_weight, preferred_element_type=jnp.float32)
    projected = projected.reshape(deep, rows, width)
    attention = projected[0]
    for k in range(1, deep):
        attention = attention + swap(projected[k].astype(jnp.bfloat16), "expert", k).astype(
            jnp.float32
        )
    middle = residual[0].astype(jnp.float32) + attention
    normed = (
        middle * lax.rsqrt(jnp.mean(middle * middle, axis=1, keepdims=True) + 1e-05) * norm_gain
    ).astype(jnp.bfloat16)

    route = route_weights[0]
    high = route.astype(jnp.bfloat16)
    rest = route - high.astype(jnp.float32)
    middle_part = rest.astype(jnp.bfloat16)
    low = (rest - middle_part.astype(jnp.float32)).astype(jnp.bfloat16)
    extra = jnp.concatenate([expert_index[0].astype(jnp.bfloat16), high, middle_part, low], axis=1)
    extra = jnp.pad(extra, ((0, 0), (0, EXTRA - extra.shape[1])))
    payload = jnp.concatenate([normed, extra], axis=1)

    pieces = []
    for k in range(deep):
        mine = gather_attn(payload if k == 0 else swap(payload, "expert", k))
        pieces.append(mine)
        for h in range(1, cores):
            pieces.append(swap(mine, "hid", h))
    tokens = jnp.stack(pieces)
    groups = deep * cores
    group_rows = wide * rows

    local_experts = gate_up_weight.shape[0]
    capacity = max(2, 2 * (rows * TOP // EXPERTS))
    first = (lax.axis_index("attn") * cores + lax.axis_index("hid")) * local_experts
    wanted = (first + jnp.arange(local_experts, dtype=jnp.int32)).astype(jnp.float32)
    tail = tokens[..., width:].astype(jnp.float32)
    routed = tail[..., :TOP]
    shares = tail[..., TOP : 2 * TOP] + tail[..., 2 * TOP : 3 * TOP] + tail[..., 3 * TOP : 4 * TOP]
    match = routed[..., None] == wanted
    hits = jnp.sum(match.astype(jnp.float32), axis=-2)
    weight = jnp.sum(jnp.where(match, shares[..., None], 0.0), axis=-2)
    before = (
        jnp.arange(rows)[None, :] < jnp.arange(rows)[:, None]
    ).astype(jnp.bfloat16)
    earlier = jnp.einsum(
        "rs,gwse->gwre", before, hits.astype(jnp.bfloat16), preferred_element_type=jnp.float32
    )
    slot = jnp.arange(wide, dtype=jnp.float32)[None, :, None, None] * capacity + earlier
    slot = jnp.where(hits > 0.0, slot, -1.0).reshape(groups, group_rows, local_experts)
    weight = weight.reshape(groups, group_rows, local_experts)
    span = wide * capacity
    picked = (
        slot.transpose(0, 2, 1)[:, :, None, :]
        == jnp.arange(span, dtype=jnp.float32)[None, None, :, None]
    )
    selector = picked.astype(jnp.bfloat16).reshape(groups, local_experts * span, group_rows)
    slot_weight = jnp.sum(
        jnp.where(picked, weight.transpose(0, 2, 1)[:, :, None, :], 0.0), axis=-1
    )
    flat = tokens[..., :width].reshape(groups, group_rows, width)
    chosen_rows = jnp.einsum(
        "gst,gtd->gsd", selector, flat, preferred_element_type=jnp.float32
    ).astype(jnp.bfloat16)
    chosen_rows = (
        chosen_rows.reshape(groups, local_experts, span, width)
        .transpose(1, 0, 2, 3)
        .reshape(local_experts, groups * span, width)
    )
    hidden = gate_up_weight.shape[3]
    merged = gate_up_weight.reshape(local_experts, width, 2 * hidden)
    both = jnp.einsum("esd,edf->esf", chosen_rows, merged, preferred_element_type=jnp.float32)
    gate_half = both[..., :hidden]
    up_half = both[..., hidden:]
    activation = ((up_half + 1.0) * gate_half * jax.nn.sigmoid(1.702 * gate_half)).astype(
        jnp.bfloat16
    )
    results = jnp.einsum(
        "esf,efd->esd", activation, down_weight, preferred_element_type=jnp.float32
    )
    scale = slot_weight.transpose(1, 0, 2).reshape(local_experts, groups * span)
    results = (results * scale[..., None]).astype(jnp.bfloat16)
    results = (
        results.reshape(local_experts, groups, span, width)
        .transpose(1, 0, 2, 3)
        .reshape(groups, local_experts * span, width)
    )
    mixed = jnp.einsum("gst,gsd->gtd", selector, results, preferred_element_type=jnp.float32)
    mixed = mixed.reshape(deep, cores, wide, rows, width)

    total = middle
    for k in reversed(range(deep)):
        part = mixed[k, 0]
        for h in range(1, cores):
            part = part + swap(mixed[k, h].astype(jnp.bfloat16), "hid", h).astype(jnp.float32)
        part = scatter_attn(part)
        if k:
            part = swap(part.astype(jnp.bfloat16), "expert", k).astype(jnp.float32)
        total = total + part
    return total.astype(jnp.bfloat16)[None]


def solution(mesh):
    in_specs = (
        P(("attn", "hid"), "expert", None),
        P(("attn", "hid"), "expert"),
        P(("attn", "hid"), "expert", None, None),
        P(("attn", "hid"), "expert", None),
        P(("attn", "hid")),
        P("expert"),
        P("expert", None),
        P(),
        P(("attn", "hid"), "expert", None),
        P(("attn", "hid"), "expert", None),
        P(("attn", "hid"), None, None, "expert"),
        P(("attn", "hid"), "expert", None),
    )
    out_specs = P(("attn", "hid"), "expert", None)
    return jax.shard_map(
        on_device, mesh=mesh, in_specs=in_specs, out_specs=out_specs, check_vma=False
    )
```

```python
import math

import jax
import jax.numpy as jnp
from jax import lax
from jax.experimental import pallas as pl
from jax.experimental.pallas import tpu as pltpu
from jax.sharding import PartitionSpec as P

EXPERTS = 32
TOP = 4
EXTRA = 64
VMEM_LIMIT = 60 * 1024 * 1024


def attend(queries, cache_pairs, fresh_pairs, cache_lengths, sink_logits):
    seq_count, kv_heads, window_slots, doubled = cache_pairs.shape
    head_dim = doubled // 2
    group_size = queries.shape[1] // (kv_heads * head_dim)
    grouped = queries.reshape(seq_count, kv_heads, group_size, head_dim)
    inv_root = 1.0 / math.sqrt(head_dim)
    scores = (
        jnp.einsum(
            "sjgd,sjtd->sjgt",
            grouped,
            cache_pairs[..., :head_dim],
            preferred_element_type=jnp.float32,
        )
        * inv_root
    )
    own_score = (
        jnp.einsum(
            "sjgd,sjd->sjg",
            grouped,
            fresh_pairs[..., :head_dim],
            preferred_element_type=jnp.float32,
        )
        * inv_root
    )
    filled = jnp.minimum(cache_lengths, window_slots)
    usable = (jnp.arange(window_slots, dtype=jnp.int32)[None, :] < filled[:, None])[
        :, None, None, :
    ]
    sink_bias = sink_logits.reshape(kv_heads, group_size)[None]
    largest = jnp.maximum(
        jnp.maximum(jnp.max(jnp.where(usable, scores, -jnp.inf), axis=-1), own_score), sink_bias
    )
    cache_exp = jnp.where(usable, jnp.exp(scores - largest[..., None]), 0.0)
    own_exp = jnp.exp(own_score - largest)
    denominator = jnp.sum(cache_exp, axis=-1) + own_exp + jnp.exp(sink_bias - largest)
    probabilities = (cache_exp / denominator[..., None]).astype(jnp.bfloat16)
    own_weight = (own_exp / denominator).astype(jnp.bfloat16)
    context = jnp.einsum(
        "sjgt,sjtd->sjgd",
        probabilities,
        cache_pairs[..., head_dim:],
        preferred_element_type=jnp.float32,
    )
    context = context + own_weight.astype(jnp.float32)[..., None] * fresh_pairs[
        :, :, None, head_dim:
    ].astype(jnp.float32)
    return context.astype(jnp.bfloat16).reshape(seq_count, -1)


def swap(value, axis, bits):
    size = lax.axis_size(axis)
    return lax.ppermute(value, axis, [(i, i ^ bits) for i in range(size)])


def axis_bits(axis):
    size = lax.axis_size(axis)
    return [1 << b for b in range(size.bit_length() - 1)]


def gather_attn(block):
    half = block.shape[0] // 2
    bits = axis_bits("attn")
    parts = []
    for piece, order in ((block[:half], bits), (block[half:], bits[::-1])):
        held = {0: piece}
        for bit in order:
            offsets = sorted(held)
            sent = held[0][None] if len(offsets) == 1 else jnp.stack([held[o] for o in offsets])
            got = swap(sent, "attn", bit)
            for place, o in enumerate(offsets):
                held[o ^ bit] = got[place]
        parts.append([held[o] for o in range(1 << len(bits))])
    return jnp.stack([jnp.concatenate(pair) for pair in zip(*parts)])


def scatter_attn(block):
    half = block.shape[1] // 2
    bits = axis_bits("attn")
    parts = []
    for piece, order in ((block[:, :half], bits), (block[:, half:], bits[::-1])):
        held = {o: piece[o] for o in range(piece.shape[0])}
        for bit in order:
            kept = [o for o in sorted(held) if not o & bit]
            sent = jnp.stack([held[o ^ bit].astype(jnp.bfloat16) for o in kept])
            got = swap(sent, "attn", bit)
            held = {o: held[o] + got[place].astype(jnp.float32) for place, o in enumerate(kept)}
        parts.append(held[0])
    return jnp.concatenate(parts)


def cut(size, step):
    return [(start, min(step, size - start)) for start in range(0, size, step)]


def expert_kernel(groups, rows, capacity, *refs):
    tok_refs = refs[:groups]
    first_ref, gate_up_ref, down_ref = refs[groups : groups + 3]
    out_refs = refs[groups + 3 : 2 * groups + 3]
    tok, picked_rows, results, spread, act, out_buf, gate_up, down = refs[2 * groups + 3 : 2 * groups + 11]
    tok_sem, gate_up_sem, down_sem, out_sem = refs[2 * groups + 11 :]
    local_experts, _, hidden, width = gate_up_ref.shape
    slots = gate_up.shape[0]
    group_rows = tok.shape[1]
    span = group_rows // rows * capacity
    lanes = local_experts * span
    hidden_cuts = cut(hidden, 256)
    f32, bf16 = jnp.float32, jnp.bfloat16

    def gate_up_copy(expert, slot, place):
        start, size = hidden_cuts[place]
        return pltpu.make_async_copy(
            gate_up_ref.at[expert, :, pl.ds(start, size)],
            gate_up.at[slot, :, pl.ds(start, size)],
            gate_up_sem.at[slot, place],
        )

    def down_copy(expert, slot):
        return pltpu.make_async_copy(down_ref.at[expert], down.at[slot], down_sem.at[slot])

    tok_copies = [
        pltpu.make_async_copy(tok_refs[g], tok.at[g], tok_sem.at[g]) for g in range(groups)
    ]
    for copy in tok_copies:
        copy.start()
    for slot in range(slots):
        for place in range(len(hidden_cuts)):
            gate_up_copy(slot, slot, place).start()
        down_copy(slot, slot).start()

    first = first_ref[0]
    lane = lax.broadcasted_iota(jnp.int32, (1, lanes), 1)
    lane_expert = (first + lane // span).astype(f32)
    lane_slot = (lane % span).astype(f32)
    row_a = lax.broadcasted_iota(jnp.int32, (group_rows, group_rows), 0)
    row_b = lax.broadcasted_iota(jnp.int32, (group_rows, group_rows), 1)
    before = jnp.where(
        (row_b < row_a) & (row_b >= row_a // rows * rows), 1.0, 0.0
    ).astype(bf16)
    base = (
        lax.broadcasted_iota(jnp.int32, (group_rows, 1), 0) // rows * capacity
    ).astype(f32)

    for g in range(groups):
        tok_copies[g].wait()
        tail = tok[g, :, width:].astype(f32)
        hits = jnp.zeros((group_rows, lanes), f32)
        for k in range(TOP):
            hits = hits + jnp.where(tail[:, k : k + 1] == lane_expert, 1.0, 0.0)
        earlier = jnp.dot(before, hits.astype(bf16), preferred_element_type=f32)
        chosen = jnp.where((hits > 0.0) & (base + earlier == lane_slot), 1.0, 0.0)
        spread[g] = chosen.astype(bf16)
        gathered = jnp.dot(
            chosen.T.astype(bf16), tok[g], preferred_element_type=f32
        ).astype(bf16)
        for e in range(local_experts):
            picked_rows[e, g * span : (g + 1) * span] = gathered[e * span : (e + 1) * span]

    def one_expert(e, carry):
        slot = lax.rem(e, slots)
        tail = picked_rows[e, :, width:].astype(f32)
        wanted = (first + e).astype(f32)
        share = jnp.zeros((tail.shape[0], 1), f32)
        for k in range(TOP):
            share_k = tail[:, TOP + k : TOP + k + 1]
            for part in (2, 3):
                at = part * TOP + k
                share_k = share_k + tail[:, at : at + 1]
            share = share + jnp.where(tail[:, k : k + 1] == wanted, share_k, 0.0)
        for place, (start, size) in enumerate(hidden_cuts):
            gate_up_copy(e, slot, place).wait()
            source = picked_rows[e, :, :width]
            sides = [
                lax.dot_general(
                    source,
                    gate_up[slot, side, start : start + size],
                    (((1,), (1,)), ((), ())),
                    preferred_element_type=f32,
                )
                for side in (0, 1)
            ]
            value = (sides[1] + 1.0) * sides[0] * jax.nn.sigmoid(1.702 * sides[0]) * share
            act[:, start : start + size] = value.astype(bf16)

        @pl.when(e + slots < local_experts)
        def _():
            for place in range(len(hidden_cuts)):
                gate_up_copy(e + slots, slot, place).start()

        down_copy(e, slot).wait()
        for start, size in cut(width, 512):
            value = jnp.dot(
                act[...], down[slot, :, start : start + size], preferred_element_type=f32
            ).astype(bf16)
            for g in range(groups):
                results[g, pl.ds(e * span, span), start : start + size] = value[
                    g * span : (g + 1) * span
                ]

        @pl.when(e + slots < local_experts)
        def _():
            down_copy(e + slots, slot).start()

        return carry

    lax.fori_loop(0, local_experts, one_expert, 0)

    out_copies = [
        pltpu.make_async_copy(out_buf.at[g % 2], out_refs[g], out_sem.at[g]) for g in range(groups)
    ]
    for g in range(groups):
        if g >= 2:
            out_copies[g - 2].wait()
        out_buf[g % 2] = jnp.dot(spread[g], results[g], preferred_element_type=f32).astype(bf16)
        out_copies[g].start()
    for g in range(max(0, groups - 2), groups):
        out_copies[g].wait()


def run_experts(pieces, first, gate_up_weight, down_weight, rows, capacity):
    groups = len(pieces)
    group_rows, padded = pieces[0].shape
    local_experts, _, hidden, width = gate_up_weight.shape
    span = group_rows // rows * capacity
    slots = min(2, local_experts)
    bf16 = jnp.bfloat16
    anywhere = pl.BlockSpec(memory_space=pl.ANY)
    return pl.pallas_call(
        lambda *refs: expert_kernel(groups, rows, capacity, *refs),
        name="experts",
        in_specs=[anywhere] * groups
        + [pl.BlockSpec(memory_space=pltpu.SMEM), anywhere, anywhere],
        out_specs=[anywhere] * groups,
        out_shape=[jax.ShapeDtypeStruct((group_rows, width), bf16)] * groups,
        scratch_shapes=[
            pltpu.VMEM((groups, group_rows, padded), bf16),
            pltpu.VMEM((local_experts, groups * span, padded), bf16),
            pltpu.VMEM((groups, local_experts * span, width), bf16),
            pltpu.VMEM((groups, group_rows, local_experts * span), bf16),
            pltpu.VMEM((groups * span, hidden), bf16),
            pltpu.VMEM((2, group_rows, width), bf16),
            pltpu.VMEM((slots, 2, hidden, width), bf16),
            pltpu.VMEM((slots, hidden, width), bf16),
            pltpu.SemaphoreType.DMA((groups,)),
            pltpu.SemaphoreType.DMA((slots, len(cut(hidden, 256)))),
            pltpu.SemaphoreType.DMA((slots,)),
            pltpu.SemaphoreType.DMA((groups,)),
        ],
        compiler_params=pltpu.CompilerParams(vmem_limit_bytes=VMEM_LIMIT),
        cost_estimate=pl.CostEstimate(
            flops=6 * local_experts * groups * span * hidden * width,
            bytes_accessed=6 * local_experts * hidden * width,
            transcendentals=local_experts * groups * span * hidden,
        ),
    )(*pieces, first, gate_up_weight, down_weight)


def on_device(
    residual,
    queries,
    cache_pairs,
    fresh_pairs,
    cache_lengths,
    sink_logits,
    out_weight,
    norm_gain,
    expert_index,
    route_weights,
    gate_up_weight,
    down_weight,
):
    deep = lax.axis_size("expert")
    wide = lax.axis_size("attn")
    cores = lax.axis_size("hid")
    place = lax.axis_index("expert")
    rows = residual.shape[1]
    width = residual.shape[2]

    context = attend(queries, cache_pairs, fresh_pairs, cache_lengths, sink_logits)
    by_place = context.reshape(deep, rows, -1)
    ordered = jnp.concatenate(
        [lax.dynamic_slice_in_dim(by_place, place ^ k, 1, 0) for k in range(deep)]
    ).reshape(deep * rows, -1)
    projected = jnp.dot(ordered, out_weight, preferred_element_type=jnp.float32)
    projected = projected.reshape(deep, rows, width)
    attention = projected[0]
    for k in range(1, deep):
        attention = attention + swap(projected[k].astype(jnp.bfloat16), "expert", k).astype(
            jnp.float32
        )
    middle = residual[0].astype(jnp.float32) + attention
    normed = (
        middle * lax.rsqrt(jnp.mean(middle * middle, axis=1, keepdims=True) + 1e-05) * norm_gain
    ).astype(jnp.bfloat16)

    route = route_weights[0]
    high = route.astype(jnp.bfloat16)
    rest = route - high.astype(jnp.float32)
    middle_part = rest.astype(jnp.bfloat16)
    low = (rest - middle_part.astype(jnp.float32)).astype(jnp.bfloat16)
    extra = jnp.concatenate([expert_index[0].astype(jnp.bfloat16), high, middle_part, low], axis=1)
    extra = jnp.pad(extra, ((0, 0), (0, EXTRA - extra.shape[1])))
    payload = jnp.concatenate([normed, extra], axis=1)

    pieces = []
    for k in range(deep):
        mine = gather_attn(payload if k == 0 else swap(payload, "expert", k))
        pieces.append(mine)
        for h in range(1, cores):
            pieces.append(swap(mine, "hid", h))
    local_experts = gate_up_weight.shape[0]
    capacity = max(2, 2 * (rows * TOP // EXPERTS))
    first = (lax.axis_index("attn") * cores + lax.axis_index("hid")) * local_experts
    mixed = run_experts(
        [piece.reshape(wide * rows, -1) for piece in pieces],
        first.astype(jnp.int32).reshape(1),
        gate_up_weight.transpose(0, 2, 3, 1),
        down_weight,
        rows,
        capacity,
    )
    mixed = [value.reshape(wide, rows, width) for value in mixed]

    total = middle
    for k in reversed(range(deep)):
        part = mixed[k * cores].astype(jnp.float32)
        for h in range(1, cores):
            part = part + swap(mixed[k * cores + h], "hid", h).astype(jnp.float32)
        part = scatter_attn(part)
        if k:
            part = swap(part.astype(jnp.bfloat16), "expert", k).astype(jnp.float32)
        total = total + part
    return total.astype(jnp.bfloat16)[None]


def solution(mesh):
    in_specs = (
        P(("attn", "hid"), "expert", None),
        P(("attn", "hid"), "expert"),
        P(("attn", "hid"), "expert", None, None),
        P(("attn", "hid"), "expert", None),
        P(("attn", "hid")),
        P("expert"),
        P("expert", None),
        P(),
        P(("attn", "hid"), "expert", None),
        P(("attn", "hid"), "expert", None),
        P(("attn", "hid"), None, None, "expert"),
        P(("attn", "hid"), "expert", None),
    )
    out_specs = P(("attn", "hid"), "expert", None)
    return jax.shard_map(
        on_device, mesh=mesh, in_specs=in_specs, out_specs=out_specs, check_vma=False
    )
```

```python
import math

import jax
import jax.numpy as jnp
from jax import lax
from jax.experimental import pallas as pl
from jax.experimental.pallas import tpu as pltpu
from jax.sharding import PartitionSpec as P

EXPERTS = 32
TOP = 4
EXTRA = 64
VMEM_LIMIT = 60 * 1024 * 1024
ATTEND_LIMIT = 40 * 1024 * 1024
ATTEND_CALLS = 2


def cut(size, step):
    return [(start, min(step, size - start)) for start in range(0, size, step)]


def attend_kernel(chunk, rows, *refs):
    scalar_ref, sink_ref, query_ref, fresh_ref, cache_ref, weight_ref = refs[:6]
    out_refs = refs[6 : 6 + chunk]
    cache, weight, context, cache_sem, weight_sem = refs[6 + chunk :]
    groups, group_seqs, kv_heads, window, doubled = cache.shape
    head_dim = doubled // 2
    lanes = sink_ref.shape[1]
    heads = lanes // group_seqs
    group_size = heads // kv_heads
    extra = 16
    inv_root = 1.0 / math.sqrt(head_dim)
    per_target = groups // chunk
    f32, bf16 = jnp.float32, jnp.bfloat16

    def first_seq(g):
        return scalar_ref[g // per_target] + g % per_target * group_seqs

    def cache_copy(g):
        return pltpu.make_async_copy(
            cache_ref.at[pl.ds(first_seq(g), group_seqs)], cache.at[g], cache_sem.at[g]
        )

    for g in range(groups):
        cache_copy(g).start()
    weight_copy = pltpu.make_async_copy(weight_ref, weight, weight_sem)
    weight_copy.start()

    lane = lax.broadcasted_iota(jnp.int32, (1, lanes), 1)
    sink = sink_ref[...]
    wide_lane = lax.broadcasted_iota(jnp.int32, (head_dim, lanes), 1)
    slot = lax.broadcasted_iota(jnp.int32, (window, lanes), 0)
    top_row = lax.broadcasted_iota(jnp.int32, (extra, doubled), 0) == 0

    def one_group(g, carry):
        seq = first_seq(g)
        cache_copy(g).wait()
        filled = jnp.zeros((1, lanes), jnp.int32)
        for s in range(group_seqs):
            filled = jnp.where(lane // heads == s, scalar_ref[chunk + seq + s], filled)
        turned = query_ref[pl.ds(pl.multiple_of(seq * heads, lanes), lanes), :].astype(f32).T
        fresh = fresh_ref[
            pl.ds(pl.multiple_of(seq * kv_heads, group_seqs * kv_heads), group_seqs * kv_heads), :
        ]
        pairs, asked = [], []
        for s in range(group_seqs):
            for j in range(kv_heads):
                at = s * kv_heads + j
                new = jnp.where(top_row, fresh[at : at + 1], 0.0).astype(bf16)
                pairs.append(jnp.concatenate([cache[g, s, j], new], axis=0))
                mine = jnp.where(wide_lane // group_size == at, turned, 0.0)
                asked.append(jnp.concatenate([mine, jnp.zeros_like(mine)], axis=0).astype(bf16))
        scores = (
            jnp.dot(
                jnp.concatenate(pairs, axis=1),
                jnp.concatenate(asked, axis=0),
                preferred_element_type=f32,
            )
            * inv_root
        )
        usable = slot < filled
        cached = scores[:window]
        own = scores[window : window + 1]
        largest = jnp.max(jnp.where(usable, cached, -jnp.inf), axis=0, keepdims=True)
        largest = jnp.maximum(jnp.maximum(largest, own), sink)
        cache_exp = jnp.where(usable, jnp.exp(cached - largest), 0.0)
        own_exp = jnp.exp(own - largest)
        total = jnp.sum(cache_exp, axis=0, keepdims=True) + own_exp + jnp.exp(sink - largest)
        share = cache_exp / total
        own_share = own_exp / total
        share = share.T
        own_share = jnp.broadcast_to(own_share, (lanes, lanes)).T[:, :extra]
        for s in range(group_seqs):
            both = jnp.concatenate(
                [share[s * heads : (s + 1) * heads], own_share[s * heads : (s + 1) * heads]],
                axis=1,
            ).astype(bf16)
            value = jnp.dot(
                both,
                jnp.concatenate(pairs[s * kv_heads : (s + 1) * kv_heads], axis=1),
                preferred_element_type=f32,
            )
            for j in range(kv_heads):
                context[
                    pl.ds(
                        pl.multiple_of(g * lanes, lanes) + s * heads + j * group_size, group_size
                    ),
                    :,
                ] = value[j * group_size : (j + 1) * group_size, j * doubled : (j + 1) * doubled]
        return carry

    lax.fori_loop(0, groups, one_group, 0)

    seqs = groups * group_seqs
    columns = [
        context[pl.ds(h, seqs, stride=heads), :][:, head_dim:].astype(bf16) for h in range(heads)
    ]
    flat = jnp.concatenate(columns, axis=1)
    weight_copy.wait()
    for start, size in cut(weight.shape[0], 512):
        value = lax.dot_general(
            flat,
            weight[start : start + size],
            (((1,), (1,)), ((), ())),
            preferred_element_type=f32,
        )
        for place in range(chunk):
            out_refs[place][:, start : start + size] = value[
                place * rows : (place + 1) * rows
            ].astype(out_refs[place].dtype)


def run_attention(starts, lengths, sinks, queries, fresh, cache_pairs, weight, rows, kinds):
    seq_count, kv_heads, window, doubled = cache_pairs.shape
    heads = sinks.shape[0]
    width = weight.shape[0]
    chunk = len(kinds)
    group_seqs = min(rows, max(1, 128 // heads))
    groups = chunk * rows // group_seqs
    scalars = pl.BlockSpec(memory_space=pltpu.SMEM)
    local = pl.BlockSpec(memory_space=pltpu.VMEM)
    anywhere = pl.BlockSpec(memory_space=pltpu.HBM)
    bf16 = jnp.bfloat16
    return pl.pallas_call(
        lambda *refs: attend_kernel(chunk, rows, *refs),
        name="attend",
        in_specs=[scalars, local, local, local, anywhere, anywhere],
        out_specs=[local] * chunk,
        out_shape=[jax.ShapeDtypeStruct((rows, width), kind) for kind in kinds],
        scratch_shapes=[
            pltpu.VMEM((groups, group_seqs, kv_heads, window, doubled), bf16),
            pltpu.VMEM(weight.shape, bf16),
            pltpu.VMEM((chunk * rows * heads, doubled), jnp.float32),
            pltpu.SemaphoreType.DMA((groups,)),
            pltpu.SemaphoreType.DMA,
        ],
        compiler_params=pltpu.CompilerParams(vmem_limit_bytes=ATTEND_LIMIT),
        cost_estimate=pl.CostEstimate(
            flops=2 * chunk * rows * heads * (doubled // 2) * width * 4,
            bytes_accessed=2 * weight.size,
            transcendentals=chunk * rows * heads * window,
        ),
    )(
        jnp.concatenate([starts, lengths]),
        jnp.tile(sinks, group_seqs)[None],
        queries,
        fresh,
        cache_pairs,
        pltpu.with_memory_space_constraint(weight, pltpu.HBM),
    )


def swap(value, axis, bits):
    size = lax.axis_size(axis)
    return lax.ppermute(value, axis, [(i, i ^ bits) for i in range(size)])


def axis_bits(axis):
    size = lax.axis_size(axis)
    return [1 << b for b in range(size.bit_length() - 1)]


def gather_attn(block):
    half = block.shape[0] // 2
    bits = axis_bits("attn")
    parts = []
    for piece, order in ((block[:half], bits), (block[half:], bits[::-1])):
        held = {0: piece}
        for bit in order:
            offsets = sorted(held)
            sent = held[0][None] if len(offsets) == 1 else jnp.stack([held[o] for o in offsets])
            got = swap(sent, "attn", bit)
            for place, o in enumerate(offsets):
                held[o ^ bit] = got[place]
        parts.append([held[o] for o in range(1 << len(bits))])
    return jnp.stack([jnp.concatenate(pair) for pair in zip(*parts)])


def scatter_attn(block):
    half = block.shape[1] // 2
    bits = axis_bits("attn")
    parts = []
    for piece, order in ((block[:, :half], bits), (block[:, half:], bits[::-1])):
        held = {o: piece[o] for o in range(piece.shape[0])}
        for bit in order:
            kept = [o for o in sorted(held) if not o & bit]
            sent = jnp.stack([held[o ^ bit].astype(jnp.bfloat16) for o in kept])
            got = swap(sent, "attn", bit)
            held = {o: held[o] + got[place].astype(jnp.float32) for place, o in enumerate(kept)}
        parts.append(held[0])
    return jnp.concatenate(parts)


def expert_kernel(groups, rows, capacity, *refs):
    tok_refs = refs[:groups]
    first_ref, gate_up_ref, down_ref = refs[groups : groups + 3]
    out_refs = refs[groups + 3 : 2 * groups + 3]
    tok, picked_rows, results, spread, act, out_buf, gate_up, down = refs[2 * groups + 3 : 2 * groups + 11]
    tok_sem, gate_up_sem, down_sem, out_sem = refs[2 * groups + 11 :]
    local_experts, _, hidden, width = gate_up_ref.shape
    slots = gate_up.shape[0]
    group_rows = tok.shape[1]
    span = group_rows // rows * capacity
    lanes = local_experts * span
    hidden_cuts = cut(hidden, 256)
    f32, bf16 = jnp.float32, jnp.bfloat16

    def gate_up_copy(expert, slot, place):
        start, size = hidden_cuts[place]
        return pltpu.make_async_copy(
            gate_up_ref.at[expert, :, pl.ds(start, size)],
            gate_up.at[slot, :, pl.ds(start, size)],
            gate_up_sem.at[slot, place],
        )

    def down_copy(expert, slot):
        return pltpu.make_async_copy(down_ref.at[expert], down.at[slot], down_sem.at[slot])

    tok_copies = [
        pltpu.make_async_copy(tok_refs[g], tok.at[g], tok_sem.at[g]) for g in range(groups)
    ]
    for copy in tok_copies:
        copy.start()
    for slot in range(slots):
        for place in range(len(hidden_cuts)):
            gate_up_copy(slot, slot, place).start()
        down_copy(slot, slot).start()

    first = first_ref[0]
    lane = lax.broadcasted_iota(jnp.int32, (1, lanes), 1)
    lane_expert = (first + lane // span).astype(f32)
    lane_slot = (lane % span).astype(f32)
    row_a = lax.broadcasted_iota(jnp.int32, (group_rows, group_rows), 0)
    row_b = lax.broadcasted_iota(jnp.int32, (group_rows, group_rows), 1)
    before = jnp.where(
        (row_b < row_a) & (row_b >= row_a // rows * rows), 1.0, 0.0
    ).astype(bf16)
    base = (
        lax.broadcasted_iota(jnp.int32, (group_rows, 1), 0) // rows * capacity
    ).astype(f32)

    for g in range(groups):
        tok_copies[g].wait()
        tail = tok[g, :, width:].astype(f32)
        hits = jnp.zeros((group_rows, lanes), f32)
        for k in range(TOP):
            hits = hits + jnp.where(tail[:, k : k + 1] == lane_expert, 1.0, 0.0)
        earlier = jnp.dot(before, hits.astype(bf16), preferred_element_type=f32)
        chosen = jnp.where((hits > 0.0) & (base + earlier == lane_slot), 1.0, 0.0)
        spread[g] = chosen.astype(bf16)
        gathered = jnp.dot(
            chosen.T.astype(bf16), tok[g], preferred_element_type=f32
        ).astype(bf16)
        for e in range(local_experts):
            picked_rows[e, g * span : (g + 1) * span] = gathered[e * span : (e + 1) * span]

    def one_expert(e, carry):
        slot = lax.rem(e, slots)
        tail = picked_rows[e, :, width:].astype(f32)
        wanted = (first + e).astype(f32)
        share = jnp.zeros((tail.shape[0], 1), f32)
        for k in range(TOP):
            share_k = tail[:, TOP + k : TOP + k + 1]
            for part in (2, 3):
                at = part * TOP + k
                share_k = share_k + tail[:, at : at + 1]
            share = share + jnp.where(tail[:, k : k + 1] == wanted, share_k, 0.0)
        for place, (start, size) in enumerate(hidden_cuts):
            gate_up_copy(e, slot, place).wait()
            source = picked_rows[e, :, :width]
            sides = [
                lax.dot_general(
                    source,
                    gate_up[slot, side, start : start + size],
                    (((1,), (1,)), ((), ())),
                    preferred_element_type=f32,
                )
                for side in (0, 1)
            ]
            value = (sides[1] + 1.0) * sides[0] * jax.nn.sigmoid(1.702 * sides[0]) * share
            act[:, start : start + size] = value.astype(bf16)

        @pl.when(e + slots < local_experts)
        def _():
            for place in range(len(hidden_cuts)):
                gate_up_copy(e + slots, slot, place).start()

        down_copy(e, slot).wait()
        for start, size in cut(width, 512):
            value = jnp.dot(
                act[...], down[slot, :, start : start + size], preferred_element_type=f32
            ).astype(bf16)
            for g in range(groups):
                results[g, pl.ds(e * span, span), start : start + size] = value[
                    g * span : (g + 1) * span
                ]

        @pl.when(e + slots < local_experts)
        def _():
            down_copy(e + slots, slot).start()

        return carry

    lax.fori_loop(0, local_experts, one_expert, 0)

    out_copies = [
        pltpu.make_async_copy(out_buf.at[g % 2], out_refs[g], out_sem.at[g]) for g in range(groups)
    ]
    for g in range(groups):
        if g >= 2:
            out_copies[g - 2].wait()
        out_buf[g % 2] = jnp.dot(spread[g], results[g], preferred_element_type=f32).astype(bf16)
        out_copies[g].start()
    for g in range(max(0, groups - 2), groups):
        out_copies[g].wait()


def run_experts(pieces, first, gate_up_weight, down_weight, rows, capacity):
    groups = len(pieces)
    group_rows, padded = pieces[0].shape
    local_experts, _, hidden, width = gate_up_weight.shape
    span = group_rows // rows * capacity
    slots = min(2, local_experts)
    bf16 = jnp.bfloat16
    anywhere = pl.BlockSpec(memory_space=pltpu.HBM)
    return pl.pallas_call(
        lambda *refs: expert_kernel(groups, rows, capacity, *refs),
        name="experts",
        in_specs=[anywhere] * groups
        + [pl.BlockSpec(memory_space=pltpu.SMEM), anywhere, anywhere],
        out_specs=[anywhere] * groups,
        out_shape=[jax.ShapeDtypeStruct((group_rows, width), bf16)] * groups,
        scratch_shapes=[
            pltpu.VMEM((groups, group_rows, padded), bf16),
            pltpu.VMEM((local_experts, groups * span, padded), bf16),
            pltpu.VMEM((groups, local_experts * span, width), bf16),
            pltpu.VMEM((groups, group_rows, local_experts * span), bf16),
            pltpu.VMEM((groups * span, hidden), bf16),
            pltpu.VMEM((2, group_rows, width), bf16),
            pltpu.VMEM((slots, 2, hidden, width), bf16),
            pltpu.VMEM((slots, hidden, width), bf16),
            pltpu.SemaphoreType.DMA((groups,)),
            pltpu.SemaphoreType.DMA((slots, len(cut(hidden, 256)))),
            pltpu.SemaphoreType.DMA((slots,)),
            pltpu.SemaphoreType.DMA((groups,)),
        ],
        compiler_params=pltpu.CompilerParams(vmem_limit_bytes=VMEM_LIMIT),
        cost_estimate=pl.CostEstimate(
            flops=6 * local_experts * groups * span * hidden * width,
            bytes_accessed=6 * local_experts * hidden * width,
            transcendentals=local_experts * groups * span * hidden,
        ),
    )(*pieces, first, gate_up_weight, down_weight)


def on_device(
    residual,
    queries,
    cache_pairs,
    fresh_pairs,
    cache_lengths,
    sink_logits,
    out_weight,
    norm_gain,
    expert_index,
    route_weights,
    gate_up_weight,
    down_weight,
):
    deep = lax.axis_size("expert")
    wide = lax.axis_size("attn")
    cores = lax.axis_size("hid")
    place = lax.axis_index("expert")
    rows = residual.shape[1]
    width = residual.shape[2]

    heads = sink_logits.shape[0]
    kv_heads = cache_pairs.shape[1]
    head_dim = cache_pairs.shape[3] // 2
    asked = queries.reshape(-1, head_dim)
    fresh = fresh_pairs.astype(jnp.float32).reshape(-1, 2 * head_dim)
    projected = {}
    calls = min(ATTEND_CALLS, deep)
    for call in reversed(range(calls)):
        offsets = list(range(call * deep // calls, (call + 1) * deep // calls))
        values = run_attention(
            jnp.stack([(place ^ k) * rows for k in offsets]).astype(jnp.int32),
            cache_lengths,
            sink_logits,
            asked,
            fresh,
            cache_pairs,
            out_weight.T,
            rows,
            [jnp.bfloat16 if k else jnp.float32 for k in offsets],
        )
        projected.update(zip(offsets, values))
    attention = projected[0]
    for k in reversed(range(1, deep)):
        attention = attention + swap(projected[k], "expert", k).astype(jnp.float32)
    middle = residual[0].astype(jnp.float32) + attention
    normed = (
        middle * lax.rsqrt(jnp.mean(middle * middle, axis=1, keepdims=True) + 1e-05) * norm_gain
    ).astype(jnp.bfloat16)

    route = route_weights[0]
    high = route.astype(jnp.bfloat16)
    rest = route - high.astype(jnp.float32)
    middle_part = rest.astype(jnp.bfloat16)
    low = (rest - middle_part.astype(jnp.float32)).astype(jnp.bfloat16)
    extra = jnp.concatenate([expert_index[0].astype(jnp.bfloat16), high, middle_part, low], axis=1)
    extra = jnp.pad(extra, ((0, 0), (0, EXTRA - extra.shape[1])))
    payload = jnp.concatenate([normed, extra], axis=1)

    pieces = []
    for k in range(deep):
        mine = gather_attn(payload if k == 0 else swap(payload, "expert", k))
        pieces.append(mine)
        for h in range(1, cores):
            pieces.append(swap(mine, "hid", h))
    local_experts = gate_up_weight.shape[0]
    capacity = max(2, 2 * (rows * TOP // EXPERTS))
    first = (lax.axis_index("attn") * cores + lax.axis_index("hid")) * local_experts
    mixed = run_experts(
        [piece.reshape(wide * rows, -1) for piece in pieces],
        first.astype(jnp.int32).reshape(1),
        gate_up_weight.transpose(0, 2, 3, 1),
        down_weight,
        rows,
        capacity,
    )
    mixed = [value.reshape(wide, rows, width) for value in mixed]

    total = middle
    for k in reversed(range(deep)):
        part = mixed[k * cores].astype(jnp.float32)
        for h in range(1, cores):
            part = part + swap(mixed[k * cores + h], "hid", h).astype(jnp.float32)
        part = scatter_attn(part)
        if k:
            part = swap(part.astype(jnp.bfloat16), "expert", k).astype(jnp.float32)
        total = total + part
    return total.astype(jnp.bfloat16)[None]


def solution(mesh):
    in_specs = (
        P(("attn", "hid"), "expert", None),
        P(("attn", "hid"), "expert"),
        P(("attn", "hid"), "expert", None, None),
        P(("attn", "hid"), "expert", None),
        P(("attn", "hid")),
        P("expert"),
        P("expert", None),
        P(),
        P(("attn", "hid"), "expert", None),
        P(("attn", "hid"), "expert", None),
        P(("attn", "hid"), None, None, "expert"),
        P(("attn", "hid"), "expert", None),
    )
    out_specs = P(("attn", "hid"), "expert", None)
    return jax.shard_map(
        on_device, mesh=mesh, in_specs=in_specs, out_specs=out_specs, check_vma=False
    )
```

```python
import math

import jax
import jax.numpy as jnp
from jax import lax
from jax.experimental import pallas as pl
from jax.experimental.pallas import tpu as pltpu
from jax.sharding import PartitionSpec as P

EXPERTS = 32
TOP = 4
EXTRA = 64
VMEM_LIMIT = 60 * 1024 * 1024
ATTEND_LIMIT = 40 * 1024 * 1024
ATTEND_CALLS = 2


def cut(size, step):
    return [(start, min(step, size - start)) for start in range(0, size, step)]


def attend_kernel(chunk, rows, *refs):
    scalar_ref, sink_ref, query_ref, fresh_ref, cache_ref, weight_ref = refs[:6]
    out_refs = refs[6 : 6 + chunk]
    cache, weight, context, cache_sem, weight_sem = refs[6 + chunk :]
    groups, group_seqs, kv_heads, window, doubled = cache.shape
    head_dim = doubled // 2
    lanes = sink_ref.shape[1]
    heads = lanes // group_seqs
    group_size = heads // kv_heads
    extra = 16
    inv_root = 1.0 / math.sqrt(head_dim)
    per_target = groups // chunk
    f32, bf16 = jnp.float32, jnp.bfloat16

    def first_seq(g):
        return scalar_ref[g // per_target] + g % per_target * group_seqs

    def cache_copy(g):
        return pltpu.make_async_copy(
            cache_ref.at[pl.ds(first_seq(g), group_seqs)], cache.at[g], cache_sem.at[g]
        )

    for g in range(groups):
        cache_copy(g).start()
    weight_copy = pltpu.make_async_copy(weight_ref, weight, weight_sem)
    weight_copy.start()

    lane = lax.broadcasted_iota(jnp.int32, (1, lanes), 1)
    sink = sink_ref[...]
    wide_lane = lax.broadcasted_iota(jnp.int32, (head_dim, lanes), 1)
    slot = lax.broadcasted_iota(jnp.int32, (window, lanes), 0)
    top_row = lax.broadcasted_iota(jnp.int32, (extra, doubled), 0) == 0

    def one_group(g, carry):
        seq = first_seq(g)
        cache_copy(g).wait()
        filled = jnp.zeros((1, lanes), jnp.int32)
        for s in range(group_seqs):
            filled = jnp.where(lane // heads == s, scalar_ref[chunk + seq + s], filled)
        turned = query_ref[pl.ds(pl.multiple_of(seq * heads, lanes), lanes), :].astype(f32).T
        fresh = fresh_ref[
            pl.ds(pl.multiple_of(seq * kv_heads, group_seqs * kv_heads), group_seqs * kv_heads), :
        ]
        pairs, asked = [], []
        for s in range(group_seqs):
            for j in range(kv_heads):
                at = s * kv_heads + j
                new = jnp.where(top_row, fresh[at : at + 1], 0.0).astype(bf16)
                pairs.append(jnp.concatenate([cache[g, s, j], new], axis=0))
                mine = jnp.where(wide_lane // group_size == at, turned, 0.0)
                asked.append(jnp.concatenate([mine, jnp.zeros_like(mine)], axis=0).astype(bf16))
        scores = (
            jnp.dot(
                jnp.concatenate(pairs, axis=1),
                jnp.concatenate(asked, axis=0),
                preferred_element_type=f32,
            )
            * inv_root
        )
        usable = slot < filled
        cached = scores[:window]
        own = scores[window : window + 1]
        largest = jnp.max(jnp.where(usable, cached, -jnp.inf), axis=0, keepdims=True)
        largest = jnp.maximum(jnp.maximum(largest, own), sink)
        cache_exp = jnp.where(usable, jnp.exp(cached - largest), 0.0)
        own_exp = jnp.exp(own - largest)
        total = jnp.sum(cache_exp, axis=0, keepdims=True) + own_exp + jnp.exp(sink - largest)
        share = cache_exp / total
        own_share = own_exp / total
        share = share.T
        own_share = jnp.broadcast_to(own_share, (lanes, lanes)).T[:, :extra]
        for s in range(group_seqs):
            both = jnp.concatenate(
                [share[s * heads : (s + 1) * heads], own_share[s * heads : (s + 1) * heads]],
                axis=1,
            ).astype(bf16)
            value = jnp.dot(
                both,
                jnp.concatenate(pairs[s * kv_heads : (s + 1) * kv_heads], axis=1),
                preferred_element_type=f32,
            )
            for j in range(kv_heads):
                context[
                    pl.ds(
                        pl.multiple_of(g * lanes, lanes) + s * heads + j * group_size, group_size
                    ),
                    :,
                ] = value[j * group_size : (j + 1) * group_size, j * doubled : (j + 1) * doubled]
        return carry

    lax.fori_loop(0, groups, one_group, 0)

    seqs = groups * group_seqs
    columns = [
        context[pl.ds(h, seqs, stride=heads), :][:, head_dim:].astype(bf16) for h in range(heads)
    ]
    flat = jnp.concatenate(columns, axis=1)
    weight_copy.wait()
    for start, size in cut(weight.shape[0], 512):
        value = lax.dot_general(
            flat,
            weight[start : start + size],
            (((1,), (1,)), ((), ())),
            preferred_element_type=f32,
        )
        for place in range(chunk):
            out_refs[place][:, start : start + size] = value[
                place * rows : (place + 1) * rows
            ].astype(out_refs[place].dtype)


def run_attention(starts, lengths, sinks, queries, fresh, cache_pairs, weight, rows, kinds):
    seq_count, kv_heads, window, doubled = cache_pairs.shape
    heads = sinks.shape[0]
    width = weight.shape[0]
    chunk = len(kinds)
    group_seqs = min(rows, max(1, 128 // heads))
    groups = chunk * rows // group_seqs
    scalars = pl.BlockSpec(memory_space=pltpu.SMEM)
    local = pl.BlockSpec(memory_space=pltpu.VMEM)
    anywhere = pl.BlockSpec(memory_space=pltpu.HBM)
    bf16 = jnp.bfloat16
    return pl.pallas_call(
        lambda *refs: attend_kernel(chunk, rows, *refs),
        name="attend",
        in_specs=[scalars, local, local, local, anywhere, anywhere],
        out_specs=[local] * chunk,
        out_shape=[jax.ShapeDtypeStruct((rows, width), kind) for kind in kinds],
        scratch_shapes=[
            pltpu.VMEM((groups, group_seqs, kv_heads, window, doubled), bf16),
            pltpu.VMEM(weight.shape, bf16),
            pltpu.VMEM((chunk * rows * heads, doubled), jnp.float32),
            pltpu.SemaphoreType.DMA((groups,)),
            pltpu.SemaphoreType.DMA,
        ],
        compiler_params=pltpu.CompilerParams(vmem_limit_bytes=ATTEND_LIMIT),
        cost_estimate=pl.CostEstimate(
            flops=2 * chunk * rows * heads * (doubled // 2) * width * 4,
            bytes_accessed=2 * weight.size,
            transcendentals=chunk * rows * heads * window,
        ),
    )(
        jnp.concatenate([starts, lengths]),
        jnp.tile(sinks, group_seqs)[None],
        queries,
        fresh,
        cache_pairs,
        pltpu.with_memory_space_constraint(weight, pltpu.HBM),
    )


def swap(value, axis, bits):
    size = lax.axis_size(axis)
    return lax.ppermute(value, axis, [(i, i ^ bits) for i in range(size)])


def axis_bits(axis):
    size = lax.axis_size(axis)
    return [1 << b for b in range(size.bit_length() - 1)]


def gather_attn(block):
    half = block.shape[0] // 2
    bits = axis_bits("attn")
    parts = []
    for piece, order in ((block[:half], bits), (block[half:], bits[::-1])):
        held = {0: piece}
        for bit in order:
            offsets = sorted(held)
            sent = held[0][None] if len(offsets) == 1 else jnp.stack([held[o] for o in offsets])
            got = swap(sent, "attn", bit)
            for place, o in enumerate(offsets):
                held[o ^ bit] = got[place]
        parts.append([held[o] for o in range(1 << len(bits))])
    return jnp.stack([jnp.concatenate(pair) for pair in zip(*parts)])


def scatter_attn(block, opened):
    half = block.shape[1] // 2
    bits = axis_bits("attn")
    parts = []
    for piece, order in ((block[:, :half], bits), (block[:, half:], bits[::-1])):
        held = {o: piece[o] for o in range(piece.shape[0])}
        for bit in order:
            kept = [o for o in sorted(held) if not o & bit]
            sent = jnp.stack([held[o ^ bit].astype(jnp.bfloat16) for o in kept])
            got = swap(sent, "attn", bit)
            held = {o: held[o] + got[place].astype(jnp.float32) for place, o in enumerate(kept)}
            if bit == order[0]:
                opened.append(got)
        parts.append(held[0])
    return jnp.concatenate(parts)


def expert_kernel(groups, rows, capacity, *refs):
    tok_refs = refs[:groups]
    first_ref, gate_up_ref, down_ref = refs[groups : groups + 3]
    out_refs = refs[groups + 3 : 2 * groups + 3]
    tok, picked_rows, results, spread, act, out_buf, gate_up, down = refs[2 * groups + 3 : 2 * groups + 11]
    tok_sem, gate_up_sem, down_sem, out_sem = refs[2 * groups + 11 :]
    local_experts, _, hidden, width = gate_up_ref.shape
    slots = gate_up.shape[0]
    group_rows = tok.shape[1]
    span = group_rows // rows * capacity
    lanes = local_experts * span
    hidden_cuts = cut(hidden, 1024)
    f32, bf16 = jnp.float32, jnp.bfloat16

    def gate_up_copy(expert, slot, place):
        start, size = hidden_cuts[place]
        return pltpu.make_async_copy(
            gate_up_ref.at[expert, :, pl.ds(start, size)],
            gate_up.at[slot, :, pl.ds(start, size)],
            gate_up_sem.at[slot, place],
        )

    def down_copy(expert, slot):
        return pltpu.make_async_copy(down_ref.at[expert], down.at[slot], down_sem.at[slot])

    tok_copies = [
        pltpu.make_async_copy(tok_refs[g], tok.at[g], tok_sem.at[g]) for g in range(groups)
    ]
    for copy in tok_copies:
        copy.start()
    for slot in range(slots):
        for place in range(len(hidden_cuts)):
            gate_up_copy(slot, slot, place).start()
        down_copy(slot, slot).start()

    first = first_ref[0]
    lane = lax.broadcasted_iota(jnp.int32, (1, lanes), 1)
    lane_expert = (first + lane // span).astype(f32)
    lane_slot = (lane % span).astype(f32)
    row_a = lax.broadcasted_iota(jnp.int32, (group_rows, group_rows), 0)
    row_b = lax.broadcasted_iota(jnp.int32, (group_rows, group_rows), 1)
    before = jnp.where(
        (row_b < row_a) & (row_b >= row_a // rows * rows), 1.0, 0.0
    ).astype(bf16)
    base = (
        lax.broadcasted_iota(jnp.int32, (group_rows, 1), 0) // rows * capacity
    ).astype(f32)

    for g in range(groups):
        tok_copies[g].wait()
        tail = tok[g, :, width:].astype(f32)
        hits = jnp.zeros((group_rows, lanes), f32)
        for k in range(TOP):
            hits = hits + jnp.where(tail[:, k : k + 1] == lane_expert, 1.0, 0.0)
        earlier = jnp.dot(before, hits.astype(bf16), preferred_element_type=f32)
        chosen = jnp.where((hits > 0.0) & (base + earlier == lane_slot), 1.0, 0.0)
        spread[g] = chosen.astype(bf16)
        gathered = jnp.dot(
            chosen.T.astype(bf16), tok[g], preferred_element_type=f32
        ).astype(bf16)
        for e in range(local_experts):
            picked_rows[e, g * span : (g + 1) * span] = gathered[e * span : (e + 1) * span]

    def one_expert(e, carry):
        slot = lax.rem(e, slots)
        tail = picked_rows[e, :, width:].astype(f32)
        wanted = (first + e).astype(f32)
        share = jnp.zeros((tail.shape[0], 1), f32)
        for k in range(TOP):
            share_k = tail[:, TOP + k : TOP + k + 1]
            for part in (2, 3):
                at = part * TOP + k
                share_k = share_k + tail[:, at : at + 1]
            share = share + jnp.where(tail[:, k : k + 1] == wanted, share_k, 0.0)
        for place, (start, size) in enumerate(hidden_cuts):
            gate_up_copy(e, slot, place).wait()
            source = picked_rows[e, :, :width]
            sides = [
                lax.dot_general(
                    gate_up[slot, side, start : start + size],
                    source,
                    (((1,), (1,)), ((), ())),
                    preferred_element_type=f32,
                )
                for side in (0, 1)
            ]
            value = (sides[1] + 1.0) * sides[0] * jax.nn.sigmoid(1.702 * sides[0])
            act[:, start : start + size] = (value.T * share).astype(bf16)

        @pl.when(e + slots < local_experts)
        def _():
            for place in range(len(hidden_cuts)):
                gate_up_copy(e + slots, slot, place).start()

        down_copy(e, slot).wait()
        for start, size in cut(width, 512):
            value = jnp.dot(
                act[...], down[slot, :, start : start + size], preferred_element_type=f32
            ).astype(bf16)
            for g in range(groups):
                results[g, pl.ds(e * span, span), start : start + size] = value[
                    g * span : (g + 1) * span
                ]

        @pl.when(e + slots < local_experts)
        def _():
            down_copy(e + slots, slot).start()

        return carry

    lax.fori_loop(0, local_experts, one_expert, 0)

    out_copies = [
        pltpu.make_async_copy(out_buf.at[g % 2], out_refs[g], out_sem.at[g]) for g in range(groups)
    ]
    for g in range(groups):
        if g >= 2:
            out_copies[g - 2].wait()
        out_buf[g % 2] = jnp.dot(spread[g], results[g], preferred_element_type=f32).astype(bf16)
        out_copies[g].start()
    for g in range(max(0, groups - 2), groups):
        out_copies[g].wait()


def run_experts(pieces, first, gate_up_weight, down_weight, rows, capacity):
    groups = len(pieces)
    group_rows, padded = pieces[0].shape
    local_experts, _, hidden, width = gate_up_weight.shape
    span = group_rows // rows * capacity
    slots = min(2, local_experts)
    bf16 = jnp.bfloat16
    anywhere = pl.BlockSpec(memory_space=pltpu.HBM)
    return pl.pallas_call(
        lambda *refs: expert_kernel(groups, rows, capacity, *refs),
        name="experts",
        in_specs=[anywhere] * groups
        + [pl.BlockSpec(memory_space=pltpu.SMEM), anywhere, anywhere],
        out_specs=[anywhere] * groups,
        out_shape=[jax.ShapeDtypeStruct((group_rows, width), bf16)] * groups,
        scratch_shapes=[
            pltpu.VMEM((groups, group_rows, padded), bf16),
            pltpu.VMEM((local_experts, groups * span, padded), bf16),
            pltpu.VMEM((groups, local_experts * span, width), bf16),
            pltpu.VMEM((groups, group_rows, local_experts * span), bf16),
            pltpu.VMEM((groups * span, hidden), bf16),
            pltpu.VMEM((2, group_rows, width), bf16),
            pltpu.VMEM((slots, 2, hidden, width), bf16),
            pltpu.VMEM((slots, hidden, width), bf16),
            pltpu.SemaphoreType.DMA((groups,)),
            pltpu.SemaphoreType.DMA((slots, len(cut(hidden, 1024)))),
            pltpu.SemaphoreType.DMA((slots,)),
            pltpu.SemaphoreType.DMA((groups,)),
        ],
        compiler_params=pltpu.CompilerParams(vmem_limit_bytes=VMEM_LIMIT),
        cost_estimate=pl.CostEstimate(
            flops=6 * local_experts * groups * span * hidden * width,
            bytes_accessed=6 * local_experts * hidden * width,
            transcendentals=local_experts * groups * span * hidden,
        ),
    )(*pieces, first, gate_up_weight, down_weight)


def on_device(
    residual,
    queries,
    cache_pairs,
    fresh_pairs,
    cache_lengths,
    sink_logits,
    out_weight,
    norm_gain,
    expert_index,
    route_weights,
    gate_up_weight,
    down_weight,
):
    deep = lax.axis_size("expert")
    wide = lax.axis_size("attn")
    cores = lax.axis_size("hid")
    place = lax.axis_index("expert")
    rows = residual.shape[1]
    width = residual.shape[2]

    heads = sink_logits.shape[0]
    kv_heads = cache_pairs.shape[1]
    head_dim = cache_pairs.shape[3] // 2
    asked = queries.reshape(-1, head_dim)
    fresh = fresh_pairs.astype(jnp.float32).reshape(-1, 2 * head_dim)
    projected = {}
    calls = min(ATTEND_CALLS, deep)
    for call in reversed(range(calls)):
        offsets = list(range(call * deep // calls, (call + 1) * deep // calls))
        values = run_attention(
            jnp.stack([(place ^ k) * rows for k in offsets]).astype(jnp.int32),
            cache_lengths,
            sink_logits,
            asked,
            fresh,
            cache_pairs,
            out_weight.T,
            rows,
            [jnp.bfloat16 if k else jnp.float32 for k in offsets],
        )
        projected.update(zip(offsets, values))
    attention = projected[0]
    for k in reversed(range(1, deep)):
        attention = attention + swap(projected[k], "expert", k).astype(jnp.float32)
    middle = residual[0].astype(jnp.float32) + attention
    normed = (
        middle * lax.rsqrt(jnp.mean(middle * middle, axis=1, keepdims=True) + 1e-05) * norm_gain
    ).astype(jnp.bfloat16)

    route = route_weights[0]
    high = route.astype(jnp.bfloat16)
    rest = route - high.astype(jnp.float32)
    middle_part = rest.astype(jnp.bfloat16)
    low = (rest - middle_part.astype(jnp.float32)).astype(jnp.bfloat16)
    extra = jnp.concatenate([expert_index[0].astype(jnp.bfloat16), high, middle_part, low], axis=1)
    extra = jnp.pad(extra, ((0, 0), (0, EXTRA - extra.shape[1])))
    payload = jnp.concatenate([normed, extra], axis=1)

    pieces = []
    blocks = [payload]
    for k in range(1, deep):
        blocks.append(swap(blocks[k & (k - 1)], "expert", k & -k))
    for k in range(deep):
        mine = gather_attn(blocks[k])
        pieces.append(mine)
        for h in range(1, cores):
            pieces.append(swap(mine, "hid", h))
    local_experts = gate_up_weight.shape[0]
    capacity = max(2, 2 * (rows * TOP // EXPERTS))
    first = (lax.axis_index("attn") * cores + lax.axis_index("hid")) * local_experts
    mixed = run_experts(
        [piece.reshape(wide * rows, -1) for piece in pieces],
        first.astype(jnp.int32).reshape(1),
        gate_up_weight.transpose(0, 2, 3, 1),
        down_weight,
        rows,
        capacity,
    )
    mixed = [value.reshape(wide, rows, width) for value in mixed]

    sums, opened = {}, {}
    for k in reversed(range(deep)):
        part = mixed[k * cores].astype(jnp.float32)
        for h in range(1, cores):
            part = part + swap(mixed[k * cores + h], "hid", h).astype(jnp.float32)
        if k + 3 < deep:
            part = lax.optimization_barrier((part, opened[k + 3]))[0]
        opened[k] = []
        sums[k] = scatter_attn(part, opened[k])
    total = middle + sums[0]
    for k in reversed(range(1, deep)):
        total = total + swap(sums[k].astype(jnp.bfloat16), "expert", k).astype(jnp.float32)
    return total.astype(jnp.bfloat16)[None]


def solution(mesh):
    in_specs = (
        P(("attn", "hid"), "expert", None),
        P(("attn", "hid"), "expert"),
        P(("attn", "hid"), "expert", None, None),
        P(("attn", "hid"), "expert", None),
        P(("attn", "hid")),
        P("expert"),
        P("expert", None),
        P(),
        P(("attn", "hid"), "expert", None),
        P(("attn", "hid"), "expert", None),
        P(("attn", "hid"), None, None, "expert"),
        P(("attn", "hid"), "expert", None),
    )
    out_specs = P(("attn", "hid"), "expert", None)
    return jax.shard_map(
        on_device, mesh=mesh, in_specs=in_specs, out_specs=out_specs, check_vma=False
    )
```
